32 devices in a mesh: tp: 2 (over x), dp: 4 (over z), dq: 4 (over y, core).
Axes of the slice: x: 2, y: 2, z: 4, core: 2. Of those that a mesh axis runs over, the one named last changes fastest.
Arguments:
- tokens: bfloat16 [16, 512, 768], P(('dp', 'dq')), may hold values from -6 to 6
- lengths: int32 [16], P(('dp', 'dq')), may hold values from 10 to 512, as said below
- weight_qkv: bfloat16 [768, 3, 768], P(None, None, 'tp'), may hold values from -0.21875 to 0.21875
- weight_out: bfloat16 [768, 768], P('tp'), may hold values from -0.875 to 0.875
- gain_one: float32 [768], replicated, may hold values from 0.25 to 1.75
- bias_one: float32 [768], replicated, may hold values from -3 to 3
- weight_up: bfloat16 [768, 3072], P(None, 'tp'), may hold values from -0.21875 to 0.21875
- weight_down: bfloat16 [3072, 768], P('tp'), may hold values from -0.15625 to 0.15625
- gain_two: float32 [768], replicated, may hold values from 0.25 to 1.75
- bias_two: float32 [768], replicated, may hold values from -3 to 3
- cotangent: bfloat16 [16, 512, 768], P(('dp', 'dq')), may hold values from -6 to 6
Outputs:
- layer_out: bfloat16 [16, 512, 768], P(('dp', 'dq'))
- grad_tokens: bfloat16 [16, 512, 768], P(('dp', 'dq'))
- grad_weight_qkv: float32 [768, 3, 768], P(None, None, 'tp')
- grad_weight_out: float32 [768, 768], P('tp')
- grad_gain_one: float32 [768], replicated
- grad_bias_one: float32 [768], replicated
- grad_weight_up: float32 [768, 3072], P(None, 'tp')
- grad_weight_down: float32 [3072, 768], P('tp')
- grad_gain_two: float32 [768], replicated
- grad_bias_two: float32 [768], replicated
The draws below stay inside these ranges and needn't reach their ends.
Inputs may be any that keep to these rules, and one draw needn't show every extreme that they name: `lengths`: real tokens of each pair; its rows from that count to 512 are padding keys. Heavy-tailed: most pairs are short; some pair has exactly 512 and some exactly 10.
All inputs are finite; a program needn't handle non-finite values.
Results may differ from the reference program's by a relative error of at most 0.018.
Values may be sent and summed in bfloat16 or wider, within the bound.
A program may use at most 128 MiB of HBM per device.

```python
import jax
import jax.numpy as jnp
from jax import lax

D = 768
HEADS = 12
HEAD_DIM = 64
FF = 3072
LEN = 512
BATCH = 16


def draw_lengths(key, part):
    key_one, key_two, key_three = jax.random.split(key, 3)
    draws_int = jax.random.randint(key_one, (BATCH,), 0, 1001)
    result = 10 + (LEN - 10) * draws_int * draws_int // 1000000
    longest = jax.random.randint(key_two, (), 0, BATCH)
    offset = jax.random.randint(key_three, (), 1, BATCH)
    shortest = (longest + offset) % BATCH
    result = result.at[longest].set(LEN).at[shortest].set(10)
    return result.astype(jnp.int32)


def steps_of(rng, shape, cuts, smallest, high):
    gain, own = 1.0, jax.random.fold_in(rng, 6)
    for axis_at, parts in cuts:
        heights = jnp.exp(jax.random.uniform(jax.random.fold_in(own, axis_at), (parts,), jnp.float32, smallest / len(cuts), high / len(cuts)))
        gain = gain * jnp.repeat(heights, shape[axis_at] // parts).reshape([-1 if axis == axis_at else 1 for axis in range(len(shape))])
    return gain


def gaussian(stream_key, extent, spread, reach, shards=(), kind=jnp.bfloat16):
    array = jax.random.normal(stream_key, extent, jnp.float32) * spread
    if len(shards) > 0:
        array = steps_of(stream_key, extent, shards, -0.22, 0.18) * array
    return jnp.clip(array, min=-reach, max=reach).astype(kind)


def setup_inputs(seed: int = 0) -> dict:
    streams_of = jax.random.split(jax.random.key(seed), 12)
    return {
        "tokens": gaussian(streams_of[0], (BATCH, LEN, D), 1.0, 6.0, ((0, 16),)),
        "lengths": draw_lengths(jax.random.fold_in(streams_of[11], 71), 0),
        "weight_qkv": gaussian(streams_of[2], (D, 3, D), D ** -0.5, 0.21875, ((2, 2),)),
        "weight_out": gaussian(streams_of[3], (D, D), (D // 16) ** -0.5, 0.875, ((0, 2),)),
        "gain_one": jnp.clip(1.0 + 0.15 * jax.random.normal(streams_of[4], (D,), jnp.float32), 0.25, 1.75),
        "bias_one": gaussian(streams_of[5], (D,), 0.5, 3.0, (), jnp.float32),
        "weight_up": gaussian(streams_of[6], (D, FF), D ** -0.5, 0.21875, ((1, 2),)),
        "weight_down": gaussian(streams_of[7], (FF, D), (FF // 2) ** -0.5, 0.15625, ((0, 2),)),
        "gain_two": jnp.clip(1.0 + 0.15 * jax.random.normal(streams_of[8], (D,), jnp.float32), 0.25, 1.75),
        "bias_two": gaussian(streams_of[9], (D,), 0.5, 3.0, (), jnp.float32),
        "cotangent": gaussian(streams_of[10], (BATCH, LEN, D), 1.0, 6.0, ((0, 16),)),
    }


@jax.custom_vjp
def low(v):
    return lax.optimization_barrier(v.astype(jnp.bfloat16)).astype(jnp.float32)

@jax.custom_vjp
def low_back(v):
    return v

def low_keep(v):
    return (low(v), None)

def low_pass(kept, grad):
    return (grad,)

def back_keep(v):
    return (v, None)

def back_low(kept, grad):
    return (low(grad),)
low.defvjp(low_keep, low_pass)
low_back.defvjp(back_keep, back_low)
epsilon = 1e-05

def matmul(left, right):
    return jnp.dot(left, right, precision=lax.Precision.HIGHEST, preferred_element_type=jnp.float32)

def gelu_exact(values):
    return 0.5 * values * (1.0 + lax.erf(values * 0.7071067811865476))

def layer_norm(values, gain_vec, bias_vec):
    centred = values - lax.optimization_barrier(jnp.mean(values, axis=-1, keepdims=True))
    variance = lax.optimization_barrier(jnp.mean(centred * centred, axis=-1, keepdims=True))
    return centred * lax.rsqrt(variance + epsilon) * gain_vec + bias_vec

def attend_one(element):
    packed_seq, length = element
    queries = packed_seq[:, 0]
    key_rows = packed_seq[:, 1]
    val_rows = packed_seq[:, 2]
    scores = jnp.einsum('qhe,khe->hqk', queries, key_rows, precision=lax.Precision.HIGHEST)
    scores = low_back(scores * HEAD_DIM ** (-0.5))
    key_live = jnp.arange(LEN, dtype=jnp.int32) < length
    scores = jnp.where(key_live[None, None, :], scores, -1000000000.0)
    shifted = scores - lax.optimization_barrier(jnp.max(scores, axis=-1, keepdims=True))
    expo = jnp.exp(shifted)
    probs = expo / lax.optimization_barrier(jnp.sum(expo, axis=-1, keepdims=True))
    return jnp.einsum('hqk,khe->qhe', low(probs), val_rows, precision=lax.Precision.HIGHEST)

def forward_group(inputs, params, length_group):
    weight_qkv, weight_out, gain_one, bias_one, weight_up, weight_down, gain_two, bias_two = params
    group_count = inputs.shape[0]
    token_rows = inputs.reshape(-1, D)
    packed = matmul(token_rows, weight_qkv.reshape(D, 3 * D))
    packed = low(low_back(packed)).reshape(group_count, LEN, 3, HEADS, HEAD_DIM)
    attended = lax.map(jax.checkpoint(attend_one), (packed, length_group))
    attended = low(low_back(attended)).reshape(-1, D)
    branch = low_back(matmul(attended, weight_out))
    normed = layer_norm(token_rows + branch, gain_one, bias_one)
    upward = low_back(matmul(low(normed), weight_up))
    activated = low(gelu_exact(upward))
    downward = low_back(matmul(activated, weight_down))
    output = layer_norm(normed + downward, gain_two, bias_two)
    return output.reshape(group_count, LEN, D)

def reference(tokens, lengths, weight_qkv, weight_out, gain_one, bias_one, weight_up, weight_down, gain_two, bias_two, cotangent):
    group_size = 1
    for attempt in range(1, 4096 // LEN + 1):
        if BATCH % attempt == 0:
            group_size = attempt
    step_total = BATCH // group_size
    params = (weight_qkv.astype(jnp.float32), weight_out.astype(jnp.float32), gain_one.astype(jnp.float32), bias_one.astype(jnp.float32), weight_up.astype(jnp.float32), weight_down.astype(jnp.float32), gain_two.astype(jnp.float32), bias_two.astype(jnp.float32))
    token_groups = tokens.astype(jnp.float32).reshape(step_total, group_size, LEN, D)
    cot_groups = cotangent.astype(jnp.float32).reshape(step_total, group_size, LEN, D)
    length_groups = lengths.astype(jnp.int32).reshape(step_total, group_size)

    def step_fn(totals, element):
        group_tokens, group_cot, group_len = element
        outputs, pullback = jax.vjp(lambda inputs, weights: forward_group(inputs, weights, group_len), group_tokens, params)
        grad_in, grad_params = pullback(group_cot)
        totals = jax.tree.map(lambda running, added: running + added, totals, grad_params)
        return (totals, (outputs.astype(jnp.bfloat16), grad_in.astype(jnp.bfloat16)))
    zeros = jax.tree.map(lambda member: jnp.zeros(member.shape, jnp.float32), params)
    totals, (outputs, grads_in) = lax.scan(step_fn, zeros, (token_groups, cot_groups, length_groups))
    layer_out = outputs.reshape(BATCH, LEN, D)
    grad_tokens = grads_in.reshape(BATCH, LEN, D)
    return (layer_out, grad_tokens, totals[0], totals[1], totals[2], totals[3], totals[4], totals[5], totals[6], totals[7])
```

```python
import functools

import jax
import jax.numpy as jnp
from jax import lax
from jax.experimental import pallas as pl
from jax.experimental.pallas import tpu as pltpu
from jax.sharding import PartitionSpec as P

HEAD_DIM = 64
EPSILON = 1e-05
MESH = pl.DeviceIdType.MESH
BF16 = jnp.bfloat16
F32 = jnp.float32
ANY = pl.BlockSpec(memory_space=pl.ANY)
VMEM_LIMIT = 63 * 2**20

CHUNK = 128
SUB = 384
SMALL = 64


def dot(left, right, left_dim, right_dim):
    return lax.dot_general(
        left, right, (((left_dim,), (right_dim,)), ((), ())), preferred_element_type=F32
    )


def row_mean(values):
    return jnp.sum(values, axis=-1, keepdims=True) * (1.0 / values.shape[-1])


def norm_forward(values):
    centred = values - row_mean(values)
    inverse = lax.rsqrt(row_mean(centred * centred) + EPSILON)
    return centred * inverse, inverse


def norm_backward(scaled, unit, inverse):
    return inverse * (scaled - row_mean(scaled) - unit * row_mean(scaled * unit))


class Layout:
    def __init__(self, width, qkv_cols, hidden):
        assert width == 2 * SUB and qkv_cols == SUB and hidden % SUB == 0
        self.subs = []
        start = 0
        for name, count, rows in (
            ("down", hidden // SUB, SUB),
            ("up", hidden // SUB, SUB),
            ("out", 1, SUB + SMALL),
            ("qkv", qkv_cols // 128, SUB),
        ):
            for index in range(count):
                self.subs.append((name, index, start, rows))
                start += rows
        self.rows = start


def layer_kernel(
    length_ref,
    tokens_hbm,
    wqkv_hbm,
    wout_hbm,
    gain_one_ref,
    bias_one_ref,
    wup_hbm,
    wdown_hbm,
    gain_two_ref,
    bias_two_ref,
    cot_hbm,
    out_hbm,
    grad_hbm,
    parts_hbm,
    tokens,
    cot,
    wqkv,
    wout,
    wup,
    wdown,
    packed,
    probs,
    attended,
    mine,
    theirs,
    unit_one,
    inv_one,
    normed,
    normed_low,
    slope,
    activated,
    grad_up_in,
    grad_res,
    grad_low,
    grad_att,
    grad_key,
    grad_val,
    grad_packed,
    small,
    parts,
    in_sem,
    out_sem,
    send_sem,
    recv_sem,
    *,
    layout,
):
    rows, width = tokens.shape
    hidden = wup.shape[1]
    cols = wout.shape[0]
    pairs = cols // 128
    chunks = rows // CHUNK
    scaling = HEAD_DIM**-0.5
    other = {"tp": 1 - lax.axis_index("tp")}

    barrier = pltpu.get_barrier_semaphore()
    pl.semaphore_signal(barrier, 1, device_id=other, device_id_type=MESH)

    loads = [
        pltpu.make_async_copy(source, target, in_sem.at[place])
        for place, (source, target) in enumerate(
            (
                (tokens_hbm, tokens),
                (wqkv_hbm, wqkv),
                (wout_hbm, wout),
                (wup_hbm, wup),
                (wdown_hbm, wdown),
                (cot_hbm, cot),
            )
        )
    ]
    for load in loads:
        load.start()

    def at(index):
        return pl.ds(pl.multiple_of(index * CHUNK, CHUNK), CHUNK)

    def exchange(which, index):
        return pltpu.make_async_remote_copy(
            src_ref=mine.at[which, at(index)],
            dst_ref=theirs.at[which, at(index)],
            send_sem=send_sem.at[which, index],
            recv_sem=recv_sem.at[which, index],
            device_id=other,
            device_id_type=MESH,
        )

    def received(which, index):
        place = at(index)
        return mine[which, place, :].astype(F32) + theirs[which, place, :].astype(F32)

    small[...] = jnp.zeros_like(small)
    grad_key[...] = jnp.zeros_like(grad_key)
    grad_val[...] = jnp.zeros_like(grad_val)

    lane = lax.broadcasted_iota(jnp.int32, (1, 128), 1)
    first = jnp.where(lane < HEAD_DIM, 1.0, 0.0).astype(BF16)
    second = jnp.where(lane < HEAD_DIM, 0.0, 1.0).astype(BF16)
    live = lax.broadcasted_iota(jnp.int32, (1, rows), 1) < length_ref[0]

    def stacked(block):
        return jnp.concatenate([block * first, block * second], axis=0)

    def merged(both):
        return jnp.where(lane < HEAD_DIM, both[:CHUNK], both[CHUNK:])

    loads[0].wait()
    loads[1].wait()

    def project(index, carry):
        place = at(index)
        for part in range(3):
            value = dot(tokens[place, :], wqkv[part], 1, 0).astype(BF16)
            packed[part, place, :] = value * BF16(scaling) if part == 0 else value
        return carry

    lax.fori_loop(0, chunks, project, 0)
    loads[2].wait()
    pl.semaphore_wait(barrier, 1)

    def attend(index, carry):
        place = at(index)
        for pair in range(pairs):
            span = slice(pair * 128, pair * 128 + 128)
            scores = dot(stacked(packed[0, place, span]), packed[1, :, span], 1, 1)
            scores = jnp.where(live, scores, -1000000000.0)
            expo = jnp.exp(scores - jnp.max(scores, axis=-1, keepdims=True))
            total = jnp.sum(expo, axis=-1, keepdims=True)
            low = (expo * (1.0 / total)).astype(BF16)
            probs[pair * chunks + index] = low
            attended[place, span] = merged(dot(low, packed[2, :, span], 1, 0)).astype(BF16)
        mine[0, place, :] = dot(attended[place, :], wout[...], 1, 0).astype(BF16)
        exchange(0, index).start()
        return carry

    lax.fori_loop(0, chunks, attend, 0)
    loads[3].wait()
    loads[4].wait()
    loads[5].wait()

    def feed(index, carry):
        place = at(index)
        exchange(0, index).wait()
        unit, inverse = norm_forward(tokens[place, :].astype(F32) + received(0, index))
        unit_one[place, :] = unit
        inv_one[place, :] = inverse
        value = unit * gain_one_ref[...] + bias_one_ref[...]
        normed[place, :] = value
        normed_low[place, :] = value.astype(BF16)
        for start in range(0, hidden, SUB):
            span = slice(start, start + SUB)
            upward = dot(normed_low[place, :], wup[:, span], 1, 0)
            share = 0.5 + 0.5 * lax.erf(upward * 0.7071067811865476)
            activated[place, span] = (upward * share).astype(BF16)
            slope[place, span] = share + upward * jnp.exp(upward * upward * -0.5) * 0.3989422804014327
        mine[1, place, :] = dot(activated[place, :], wdown[...], 1, 0).astype(BF16)
        exchange(1, index).start()
        return carry

    lax.fori_loop(0, chunks, feed, 0)

    def turn(index, carry):
        place = at(index)
        exchange(1, index).wait()
        unit, inverse = norm_forward(normed[place, :] + received(1, index))
        mine[2, place, :] = (unit * gain_two_ref[...] + bias_two_ref[...]).astype(BF16)
        pltpu.make_async_copy(mine.at[2, place], out_hbm.at[place], out_sem.at[0, index]).start()
        flow = cot[place, :].astype(F32)
        small[2:3, :] += jnp.sum(flow * unit, axis=0, keepdims=True)
        small[3:4, :] += jnp.sum(flow, axis=0, keepdims=True)
        grad = norm_backward(flow * gain_two_ref[...], unit, inverse)
        grad_res[place, :] = grad
        grad_low[0, place, :] = grad.astype(BF16)
        for start in range(0, hidden, SUB):
            span = slice(start, start + SUB)
            grad_act = dot(grad_low[0, place, :], wdown[span, :], 1, 1)
            grad_up_in[place, span] = (grad_act * slope[place, span]).astype(BF16)
        mine[3, place, :] = dot(grad_up_in[place, :], wup[...], 1, 1).astype(BF16)
        exchange(3, index).start()
        return carry

    lax.fori_loop(0, chunks, turn, 0)

    for name, which, start, extent in layout.subs:
        if name == "down":
            parts[start : start + extent, :] = dot(
                activated[:, which * SUB : which * SUB + SUB], grad_low[0], 0, 0
            ).astype(BF16)
        if name == "up":
            down_at, right_at = which % 2 * SUB, which // 2 * width
            parts[start : start + extent, :] = dot(
                normed_low[:, down_at : down_at + SUB],
                grad_up_in[:, right_at : right_at + width],
                0,
                0,
            ).astype(BF16)

    def attend_back(index, carry):
        place = at(index)
        exchange(3, index).wait()
        unit = unit_one[place, :]
        flow = grad_res[place, :] + received(3, index)
        small[0:1, :] += jnp.sum(flow * unit, axis=0, keepdims=True)
        small[1:2, :] += jnp.sum(flow, axis=0, keepdims=True)
        grad = norm_backward(flow * gain_one_ref[...], unit, inv_one[place, :])
        grad_res[place, :] = grad
        grad_low[1, place, :] = grad.astype(BF16)
        grad_att[place, :] = dot(grad_low[1, place, :], wout[...], 1, 1).astype(BF16)
        for pair in range(pairs):
            span = slice(pair * 128, pair * 128 + 128)
            low = probs[pair * chunks + index]
            pull = stacked(grad_att[place, span])
            seen = attended[place, span].astype(F32)
            centre = jnp.sum(
                pull.astype(F32) * jnp.concatenate([seen, seen], axis=0), axis=-1, keepdims=True
            )
            grad_probs = dot(pull, packed[2, :, span], 1, 1)
            grad_scores = (low.astype(F32) * (grad_probs - centre)).astype(BF16)
            grad_val[:, span] += dot(low, pull, 0, 0)
            grad_key[:, span] += dot(grad_scores, stacked(packed[0, place, span]), 0, 0)
            grad_query = merged(dot(grad_scores, packed[1, :, span], 1, 0)) * scaling
            grad_packed[0, place, span] = grad_query.astype(BF16)
        return carry

    lax.fori_loop(0, chunks, attend_back, 0)
    grad_packed[1] = grad_key[...].astype(BF16)
    grad_packed[2] = grad_val[...].astype(BF16)

    def leave(index, carry):
        place = at(index)
        total = dot(grad_packed[0, place, :], wqkv[0], 1, 1)
        total += dot(grad_packed[1, place, :], wqkv[1], 1, 1)
        total += dot(grad_packed[2, place, :], wqkv[2], 1, 1)
        mine[4, place, :] = total.astype(BF16)
        exchange(4, index).start()
        return carry

    lax.fori_loop(0, chunks, leave, 0)

    for name, which, start, extent in layout.subs:
        if name == "out":
            parts[start : start + SUB, :] = dot(attended[...], grad_low[1], 0, 0).astype(BF16)
            parts[start + SUB : start + extent, :] = small[...].astype(BF16)
        if name == "qkv":
            span = slice(which * 128, which * 128 + 128)
            for part in range(3):
                value = dot(tokens[...], grad_packed[part, :, span], 0, 0).astype(BF16)
                for half in range(2):
                    left = half * SUB + part * 128
                    parts[start : start + SUB, left : left + 128] = value[
                        half * SUB : half * SUB + SUB
                    ]

    flush = pltpu.make_async_copy(parts, parts_hbm, in_sem.at[6])
    flush.start()

    def finish(index, carry):
        place = at(index)
        exchange(4, index).wait()
        mine[5, place, :] = (grad_res[place, :] + received(4, index)).astype(BF16)
        pltpu.make_async_copy(mine.at[5, place], grad_hbm.at[place], out_sem.at[1, index]).start()
        return carry

    lax.fori_loop(0, chunks, finish, 0)

    def drain(index, carry):
        place = at(index)
        pltpu.make_async_copy(mine.at[2, place], out_hbm.at[place], out_sem.at[0, index]).wait()
        pltpu.make_async_copy(mine.at[5, place], grad_hbm.at[place], out_sem.at[1, index]).wait()
        return carry

    lax.fori_loop(0, chunks, drain, 0)
    flush.wait()


class Sum:
    def __init__(self, layout, parts, totals, near, across, inflow, middle, send_sem, recv_sem):
        self.layout, self.parts, self.totals = layout, parts, totals
        self.near, self.across, self.inflow, self.middle = near, across, inflow, middle
        self.send_sem, self.recv_sem = send_sem, recv_sem
        line, group = lax.axis_size("dp"), lax.axis_size("dq")
        assert group == 4 and line % 2 == 0
        self.spot, place = lax.axis_index("dp"), lax.axis_index("dq")
        self.core, self.chip = lax.rem(place, 2), lax.div(place, 2)
        self.even, self.odd = self.core == 0, self.core == 1
        lower = self.spot < line // 2
        self.side = jnp.where(lower, 0, 1)
        self.centre = jnp.logical_or(self.spot == line // 2 - 1, self.spot == line // 2)
        self.outer = jnp.logical_and(self.spot > 0, self.spot < line - 1)
        if line == 2:
            self.outer = self.spot < 0
        self.to_core = {"dq": place + 1 - 2 * self.core}
        self.to_chip = {"dq": lax.rem(place + 2, 4)}
        self.inward = {"dp": jnp.where(lower, self.spot + 1, self.spot - 1)}
        self.outward = {"dp": jnp.where(lower, self.spot - 1, self.spot + 1)}

    def greet(self, barrier):
        for device in (self.to_core, self.to_chip, self.inward):
            pl.semaphore_signal(barrier, 1, device_id=device, device_id_type=MESH)

        @pl.when(self.outer)
        def _():
            pl.semaphore_signal(barrier, 1, device_id=self.outward, device_id_type=MESH)

    def meet(self, barrier, more=0):
        pl.semaphore_wait(barrier, 3 + more + jnp.where(self.outer, 1, 0))

    def span(self, k, core=None, chip=None):
        _, _, start, rows = self.layout.subs[k]
        if core is None:
            return pl.ds(start, rows)
        first = start + core * (rows // 2)
        if chip is None:
            return pl.ds(pl.multiple_of(first, 16), rows // 2)
        return pl.ds(pl.multiple_of(first + chip * (rows // 4), 16), rows // 4)

    def slot(self, k, share):
        _, _, start, rows = self.layout.subs[k]
        return pl.ds(start // share, rows // share)

    def copy(self, kind, k, source, target, device):
        return pltpu.make_async_remote_copy(
            src_ref=source,
            dst_ref=target,
            send_sem=self.send_sem.at[kind, k],
            recv_sem=self.recv_sem.at[kind, k],
            device_id=device,
            device_id_type=MESH,
        )

    def add(self, place, arrived, target=None):
        value = self.parts[place, :].astype(F32) + arrived.astype(F32)
        target = self.parts if target is None else target
        target[place, :] = value.astype(BF16)

    def half(self, k):
        return self.span(k, self.core)

    def quarter(self, k, which):
        return self.span(k, self.core, which)

    def over_core(self, k):
        return self.copy(
            0, k, self.parts.at[self.span(k, 1 - self.core)], self.near.at[self.slot(k, 2)], self.to_core
        )

    def over_chip(self, k, which):
        return self.copy(
            1, k, self.parts.at[self.quarter(k, which)], self.across.at[self.slot(k, 4)], self.to_chip
        )

    def run_in(self, k, place, share):
        return self.copy(2, k, self.parts.at[place], self.inflow.at[self.slot(k, share)], self.inward)

    def swap(self, k, which):
        return self.copy(
            3, k, self.parts.at[self.quarter(k, which)], self.middle.at[self.slot(k, 4)], self.inward
        )

    def hand_on(self, kind, k, place, device):
        return self.copy(kind, k, self.totals.at[place], self.totals.at[place], device)

    def pass_even(self, k):
        mine = self.quarter(k, self.chip)

        @pl.when(self.centre)
        def _():
            self.swap(k, self.chip).start()

        @pl.when(jnp.logical_not(self.centre))
        def _():
            self.run_in(k, mine, 4).start()

    def pass_odd(self, k):
        @pl.when(self.centre)
        def _():
            self.swap(k, 1 - self.side).start()

        @pl.when(jnp.logical_not(self.centre))
        def _():
            self.run_in(k, self.half(k), 2).start()

    def stage(self, number, k):
        even, odd, centre, outer = self.even, self.odd, self.centre, self.outer
        both = jnp.logical_and
        inner = jnp.logical_not(centre)
        mine = self.quarter(k, self.chip)
        half = self.half(k)

        def when(*conditions):
            return pl.when(functools.reduce(both, conditions))

        if number == 0:
            self.over_core(k).start()
        if number == 1:
            self.over_core(k).wait()
            self.add(half, self.near[self.slot(k, 2), :])

            @when(even)
            def _():
                self.over_chip(k, 1 - self.chip).start()

            @when(odd, jnp.logical_not(outer))
            def _():
                self.pass_odd(k)

        if number == 2:

            @when(even)
            def _():
                self.over_chip(k, 1 - self.chip).wait()
                self.add(mine, self.across[self.slot(k, 4), :])

            @when(even, jnp.logical_not(outer))
            def _():
                self.pass_even(k)

            @when(odd, outer)
            def _():
                self.run_in(k, half, 2).wait_recv()
                self.add(half, self.inflow[self.slot(k, 2), :])
                self.pass_odd(k)

        if number == 3:

            @when(even, outer)
            def _():
                self.run_in(k, mine, 4).wait_recv()
                self.add(mine, self.inflow[self.slot(k, 4), :])
                self.pass_even(k)

            @when(odd, centre)
            def _():
                self.swap(k, 1 - self.side).wait()
                self.add(self.quarter(k, self.side), self.middle[self.slot(k, 4), :])
                self.over_chip(k, self.side).start()

        if number == 4:

            @when(even, centre)
            def _():
                self.swap(k, self.chip).wait()
                self.add(mine, self.middle[self.slot(k, 4), :], self.totals)

            @when(even, centre, outer)
            def _():
                self.hand_on(4, k, mine, self.outward).start()

            @when(even, centre)
            def _():
                self.hand_on(5, k, mine, self.to_chip).start()

            @when(odd, centre)
            def _():
                self.over_chip(k, self.side).wait()
                self.add(self.quarter(k, self.side), self.across[self.slot(k, 4), :], self.totals)
                self.hand_on(5, k, self.quarter(k, self.side), self.inward).start()

        if number == 5:

            @when(even, inner)
            def _():
                self.run_in(k, mine, 4).wait_send()
                self.hand_on(4, k, mine, self.inward).wait_recv()

            @when(even, inner, outer)
            def _():
                self.hand_on(4, k, mine, self.outward).start()

            @when(even, inner)
            def _():
                self.hand_on(5, k, mine, self.to_chip).start()

            @when(odd, centre)
            def _():
                self.hand_on(5, k, self.quarter(k, self.side), self.inward).wait_send()
                self.hand_on(5, k, self.quarter(k, 1 - self.side), self.inward).wait_recv()

            @when(odd, centre, outer)
            def _():
                self.hand_on(4, k, half, self.outward).start()

            @when(odd, centre)
            def _():
                self.hand_on(6, k, half, self.to_core).start()

        if number == 6:

            @when(even)
            def _():
                self.hand_on(5, k, mine, self.to_chip).wait_send()
                self.hand_on(5, k, self.quarter(k, 1 - self.chip), self.to_chip).wait_recv()
                self.hand_on(6, k, half, self.to_core).start()

            @when(odd, inner)
            def _():
                self.run_in(k, half, 2).wait_send()
                self.hand_on(4, k, half, self.inward).wait_recv()

            @when(odd, inner, outer)
            def _():
                self.hand_on(4, k, half, self.outward).start()

            @when(odd, inner)
            def _():
                self.hand_on(6, k, half, self.to_core).start()

        if number == 7:

            @when(even, outer)
            def _():
                self.hand_on(4, k, mine, self.outward).wait_send()

            @when(odd, outer)
            def _():
                self.hand_on(4, k, half, self.outward).wait_send()

            self.hand_on(6, k, half, self.to_core).wait_send()
            self.hand_on(6, k, self.span(k, 1 - self.core), self.to_core).wait_recv()


STAGES = 8


def sum_kernel(
    parts_hbm, sums_hbm, parts, totals, near, across, inflow, middle, in_sem, out_sem, send_sem, recv_sem, *, layout
):
    total = Sum(layout, parts, totals, near, across, inflow, middle, send_sem, recv_sem)
    barrier = pltpu.get_barrier_semaphore()
    total.greet(barrier)
    count = len(layout.subs)

    def load(k):
        return pltpu.make_async_copy(
            parts_hbm.at[total.span(k)], parts.at[total.span(k)], in_sem.at[k]
        )

    def store(k):
        return pltpu.make_async_copy(
            totals.at[total.span(k)], sums_hbm.at[total.span(k)], out_sem.at[k]
        )

    for k in range(count):
        load(k).start()
    total.meet(barrier)
    for step in range(count + STAGES - 1):
        for number in reversed(range(STAGES)):
            k = step - number
            if 0 <= k < count:
                if number == 0:
                    load(k).wait()
                total.stage(number, k)
                if number == STAGES - 1:
                    store(k).start()
    for k in range(count):
        store(k).wait()


def widen_kernel(
    sums_hbm,
    out_in,
    grad_in,
    out_hbm,
    grad_hbm,
    qkv_hbm,
    wout_hbm,
    gain_one_hbm,
    bias_one_hbm,
    up_hbm,
    down_hbm,
    gain_two_hbm,
    bias_two_hbm,
    sums,
    wide,
    rows_in,
    in_sem,
    out_sem,
    row_sem,
    *,
    layout,
):
    slots = wide.shape[0]
    width = sums.shape[1]

    def load(k):
        _, _, start, rows = layout.subs[k]
        return pltpu.make_async_copy(
            sums_hbm.at[pl.ds(start, rows)], sums.at[pl.ds(start, rows)], in_sem.at[k]
        )

    def stores(k):
        name, which, _, _ = layout.subs[k]
        slot = k % slots
        block = wide.at[slot, pl.ds(0, SUB)]
        if name == "down":
            pieces = [(block, down_hbm.at[pl.ds(which * SUB, SUB)])]
        elif name == "up":
            pieces = [
                (block, up_hbm.at[pl.ds(which % 2 * SUB, SUB), pl.ds(which // 2 * width, width)])
            ]
        elif name == "out":
            pieces = [(block, wout_hbm)]
            for row, target in enumerate((gain_one_hbm, bias_one_hbm, gain_two_hbm, bias_two_hbm)):
                pieces.append((wide.at[slot, pl.ds(SUB + 8 * row, 1)], target))
        else:
            pieces = [
                (
                    wide.at[slot, pl.ds(0, SUB), pl.ds(half * SUB + part * 128, 128)],
                    qkv_hbm.at[part, pl.ds(half * SUB, SUB), pl.ds(which * 128, 128)],
                )
                for half in range(2)
                for part in range(3)
            ]
        return [
            pltpu.make_async_copy(source, target, out_sem.at[slot, place])
            for place, (source, target) in enumerate(pieces)
        ]

    through = ((out_in, out_hbm), (grad_in, grad_hbm))
    for place, (source, _) in enumerate(through):
        pltpu.make_async_copy(source, rows_in.at[place], row_sem.at[place]).start()
    for k in range(len(layout.subs)):
        load(k).start()
    for place, (source, target) in enumerate(through):
        pltpu.make_async_copy(source, rows_in.at[place], row_sem.at[place]).wait()
        pltpu.make_async_copy(rows_in.at[place], target, row_sem.at[2 + place]).start()
    for k, (name, _, start, _) in enumerate(layout.subs):
        load(k).wait()
        if k >= slots:
            for store in stores(k - slots):
                store.wait()
        wide[k % slots, 0:SUB, :] = sums[start : start + SUB, :].astype(F32)
        if name == "out":
            low = sums[start + SUB : start + SUB + 16, :].astype(F32)
            for row in range(4):
                wide[k % slots, SUB + 8 * row : SUB + 8 * row + 1, :] = low[row : row + 1]
        for store in stores(k):
            store.start()
    for k in range(len(layout.subs) - slots, len(layout.subs)):
        for store in stores(k):
            store.wait()
    for place, (_, target) in enumerate(through):
        pltpu.make_async_copy(rows_in.at[place], target, row_sem.at[2 + place]).wait()


def on_device(
    tokens,
    lengths,
    weight_qkv,
    weight_out,
    gain_one,
    bias_one,
    weight_up,
    weight_down,
    gain_two,
    bias_two,
    cotangent,
):
    seq_count, rows, width = tokens.shape
    cols, hidden = weight_out.shape[0], weight_up.shape[1]
    assert seq_count == 1 and rows % CHUNK == 0 and lax.axis_size("tp") == 2
    layout = Layout(width, cols, hidden)
    count = len(layout.subs)
    chunks = rows // CHUNK
    pairs = cols // 128
    whole = pl.BlockSpec(memory_space=pltpu.VMEM)
    out_rows, grad_rows, parts = pl.pallas_call(
        functools.partial(layer_kernel, layout=layout),
        name="layer",
        out_shape=(
            jax.ShapeDtypeStruct((rows, width), BF16),
            jax.ShapeDtypeStruct((rows, width), BF16),
            jax.ShapeDtypeStruct((layout.rows, width), BF16),
        ),
        in_specs=[
            pl.BlockSpec(memory_space=pltpu.SMEM),
            ANY,
            ANY,
            ANY,
            whole,
            whole,
            ANY,
            ANY,
            whole,
            whole,
            ANY,
        ],
        out_specs=(ANY, ANY, ANY),
        scratch_shapes=[
            pltpu.VMEM((rows, width), BF16),
            pltpu.VMEM((rows, width), BF16),
            pltpu.VMEM((3, width, cols), BF16),
            pltpu.VMEM((cols, width), BF16),
            pltpu.VMEM((width, hidden), BF16),
            pltpu.VMEM((hidden, width), BF16),
            pltpu.VMEM((3, rows, cols), BF16),
            pltpu.VMEM((pairs * chunks, 2 * CHUNK, rows), BF16),
            pltpu.VMEM((rows, cols), BF16),
            pltpu.VMEM((6, rows, width), BF16),
            pltpu.VMEM((5, rows, width), BF16),
            pltpu.VMEM((rows, width), F32),
            pltpu.VMEM((rows, 1), F32),
            pltpu.VMEM((rows, width), F32),
            pltpu.VMEM((rows, width), BF16),
            pltpu.VMEM((rows, hidden), F32),
            pltpu.VMEM((rows, hidden), BF16),
            pltpu.VMEM((rows, hidden), BF16),
            pltpu.VMEM((rows, width), F32),
            pltpu.VMEM((2, rows, width), BF16),
            pltpu.VMEM((rows, cols), BF16),
            pltpu.VMEM((rows, cols), F32),
            pltpu.VMEM((rows, cols), F32),
            pltpu.VMEM((3, rows, cols), BF16),
            pltpu.VMEM((SMALL, width), F32),
            pltpu.VMEM((layout.rows, width), BF16),
            pltpu.SemaphoreType.DMA((7,)),
            pltpu.SemaphoreType.DMA((2, chunks)),
            pltpu.SemaphoreType.DMA((5, chunks)),
            pltpu.SemaphoreType.DMA((5, chunks)),
        ],
        compiler_params=pltpu.CompilerParams(
            collective_id=1, has_side_effects=True, vmem_limit_bytes=VMEM_LIMIT
        ),
    )(
        lengths,
        tokens.reshape(rows, width),
        jnp.transpose(weight_qkv, (1, 0, 2)),
        weight_out,
        gain_one.reshape(1, width),
        bias_one.reshape(1, width),
        weight_up,
        weight_down,
        gain_two.reshape(1, width),
        bias_two.reshape(1, width),
        cotangent.reshape(rows, width),
    )
    sums = pl.pallas_call(
        functools.partial(sum_kernel, layout=layout),
        name="sum",
        out_shape=jax.ShapeDtypeStruct((layout.rows, width), BF16),
        in_specs=[ANY],
        out_specs=ANY,
        scratch_shapes=[
            pltpu.VMEM((layout.rows, width), BF16),
            pltpu.VMEM((layout.rows, width), BF16),
            pltpu.VMEM((layout.rows // 2, width), BF16),
            pltpu.VMEM((layout.rows // 4, width), BF16),
            pltpu.VMEM((layout.rows // 2, width), BF16),
            pltpu.VMEM((layout.rows // 4, width), BF16),
            pltpu.SemaphoreType.DMA((count,)),
            pltpu.SemaphoreType.DMA((count,)),
            pltpu.SemaphoreType.DMA((7, count)),
            pltpu.SemaphoreType.DMA((7, count)),
        ],
        compiler_params=pltpu.CompilerParams(
            collective_id=2, has_side_effects=True, vmem_limit_bytes=VMEM_LIMIT
        ),
    )(parts)
    vector = jax.ShapeDtypeStruct((1, width), F32)
    results = pl.pallas_call(
        functools.partial(widen_kernel, layout=layout),
        name="widen",
        out_shape=(
            jax.ShapeDtypeStruct((rows, width), BF16),
            jax.ShapeDtypeStruct((rows, width), BF16),
            jax.ShapeDtypeStruct((3, width, cols), F32),
            jax.ShapeDtypeStruct((cols, width), F32),
            vector,
            vector,
            jax.ShapeDtypeStruct((width, hidden), F32),
            jax.ShapeDtypeStruct((hidden, width), F32),
            vector,
            vector,
        ),
        in_specs=[ANY] * 3,
        out_specs=(ANY,) * 10,
        scratch_shapes=[
            pltpu.VMEM((layout.rows, width), BF16),
            pltpu.VMEM((4, SUB + 32, width), F32),
            pltpu.VMEM((2, rows, width), BF16),
            pltpu.SemaphoreType.DMA((count,)),
            pltpu.SemaphoreType.DMA((4, 6)),
            pltpu.SemaphoreType.DMA((4,)),
        ],
        compiler_params=pltpu.CompilerParams(vmem_limit_bytes=VMEM_LIMIT),
    )(sums, out_rows, grad_rows)
    return (
        results[0].reshape(seq_count, rows, width),
        results[1].reshape(seq_count, rows, width),
        jnp.transpose(results[2], (1, 0, 2)),
        results[3],
        results[4].reshape(width),
        results[5].reshape(width),
        results[6],
        results[7],
        results[8].reshape(width),
        results[9].reshape(width),
    )


def solution(mesh):
    batch = P(("dp", "dq"), None, None)
    return jax.shard_map(
        on_device,
        mesh=mesh,
        in_specs=(
            batch,
            P(("dp", "dq")),
            P(None, None, "tp"),
            P("tp", None),
            P(),
            P(),
            P(None, "tp"),
            P("tp", None),
            P(),
            P(),
            batch,
        ),
        out_specs=(
            batch,
            batch,
            P(None, None, "tp"),
            P("tp", None),
            P(),
            P(),
            P(None, "tp"),
            P("tp", None),
            P(),
            P(),
        ),
        check_vma=False,
    )
```

```python
import functools

import jax
import jax.numpy as jnp
from jax import lax
from jax.experimental import pallas as pl
from jax.experimental.pallas import tpu as pltpu
from jax.sharding import PartitionSpec as P

HEAD_DIM = 64
EPSILON = 1e-05
MESH = pl.DeviceIdType.MESH
BF16 = jnp.bfloat16
F32 = jnp.float32
ANY = pl.BlockSpec(memory_space=pl.ANY)
VMEM_LIMIT = 63 * 2**20

CHUNK = 128
SUB = 384
SMALL = 64


def dot(left, right, left_dim, right_dim):
    return lax.dot_general(
        left, right, (((left_dim,), (right_dim,)), ((), ())), preferred_element_type=F32
    )


def row_mean(values):
    return jnp.sum(values, axis=-1, keepdims=True) * (1.0 / values.shape[-1])


def norm_forward(values):
    centred = values - row_mean(values)
    inverse = lax.rsqrt(row_mean(centred * centred) + EPSILON)
    return centred * inverse, inverse


def norm_backward(scaled, unit, inverse):
    return inverse * (scaled - row_mean(scaled) - unit * row_mean(scaled * unit))


class Layout:
    def __init__(self, width, qkv_cols, hidden):
        assert width == 2 * SUB and qkv_cols == SUB and hidden % SUB == 0
        self.subs = []
        start = 0
        for name, count, rows in (
            ("down", hidden // SUB, SUB),
            ("up", hidden // SUB, SUB),
            ("out", 1, SUB + SMALL),
            ("qkv", qkv_cols // 128, SUB),
        ):
            for index in range(count):
                self.subs.append((name, index, start, rows))
                start += rows
        self.rows = start


class Sum:
    def __init__(self, layout, parts, totals, near, across, inflow, middle, send_sem, recv_sem):
        self.layout, self.parts, self.totals = layout, parts, totals
        self.near, self.across, self.inflow, self.middle = near, across, inflow, middle
        self.send_sem, self.recv_sem = send_sem, recv_sem
        line, group = lax.axis_size("dp"), lax.axis_size("dq")
        assert group == 4 and line % 2 == 0
        self.spot, place = lax.axis_index("dp"), lax.axis_index("dq")
        self.core, self.chip = lax.rem(place, 2), lax.div(place, 2)
        self.even, self.odd = self.core == 0, self.core == 1
        lower = self.spot < line // 2
        self.side = jnp.where(lower, 0, 1)
        self.centre = jnp.logical_or(self.spot == line // 2 - 1, self.spot == line // 2)
        self.inner = jnp.logical_not(self.centre)
        self.outer = jnp.logical_and(self.spot > 0, self.spot < line - 1)
        self.end = jnp.logical_not(self.outer)
        self.to_core = {"dq": place + 1 - 2 * self.core}
        self.to_chip = {"dq": lax.rem(place + 2, 4)}
        self.inward = {"dp": jnp.where(lower, self.spot + 1, self.spot - 1)}
        self.outward = {"dp": jnp.where(lower, self.spot - 1, self.spot + 1)}

    def greet(self, barrier):
        for device in (self.to_core, self.to_chip, self.inward):
            pl.semaphore_signal(barrier, 1, device_id=device, device_id_type=MESH)

        @pl.when(self.outer)
        def _():
            pl.semaphore_signal(barrier, 1, device_id=self.outward, device_id_type=MESH)

    def meet(self, barrier, more=0):
        pl.semaphore_wait(barrier, 3 + more + jnp.where(self.outer, 1, 0))

    def half(self, k, core=None):
        _, _, start, rows = self.layout.subs[k]
        first = start + (self.core if core is None else core) * (rows // 2)
        return pl.ds(pl.multiple_of(first, 16), rows // 2)

    def quarter(self, k, which):
        _, _, start, rows = self.layout.subs[k]
        first = start + self.core * (rows // 2) + which * (rows // 4)
        return pl.ds(pl.multiple_of(first, 16), rows // 4)

    def slot(self, k, share):
        _, _, start, rows = self.layout.subs[k]
        return pl.ds(start // share, rows // share)

    def copy(self, sent, arrived, k, source, target, device):
        return pltpu.make_async_remote_copy(
            src_ref=source,
            dst_ref=target,
            send_sem=self.send_sem.at[sent, k],
            recv_sem=self.recv_sem.at[arrived, k],
            device_id=device,
            device_id_type=MESH,
        )

    def add(self, k, place, buffer, share, target=None):
        arrived = buffer[self.slot(k, share), :]
        value = self.parts[place, :].astype(F32) + arrived.astype(F32)
        target = self.parts if target is None else target
        target[place, :] = value.astype(BF16)

    def over_core(self, k):
        near = self.near.at[self.slot(k, 2)]
        return self.copy(0, 0, k, self.parts.at[self.half(k, 1 - self.core)], near, self.to_core)

    def over_chip(self, k, which):
        across = self.across.at[self.slot(k, 4)]
        return self.copy(1, 1, k, self.parts.at[self.quarter(k, which)], across, self.to_chip)

    def run_in(self, k, which):
        inflow = self.inflow.at[self.slot(k, 4)]
        return self.copy(2, 2, k, self.parts.at[self.quarter(k, which)], inflow, self.inward)

    def swap(self, k, which):
        middle = self.middle.at[self.slot(k, 4)]
        return self.copy(3, 3, k, self.parts.at[self.quarter(k, which)], middle, self.inward)

    def run_out(self, k, which):
        middle = self.middle.at[self.slot(k, 4)]
        return self.copy(4, 3, k, self.parts.at[self.quarter(k, which)], middle, self.outward)

    def hand_on(self, sent, arrived, k, place, device):
        total = self.totals.at[place]
        return self.copy(sent, arrived, k, total, total, device)

    def send_in(self, k, which):
        @pl.when(self.centre)
        def _():
            self.swap(k, which).start()

        @pl.when(self.inner)
        def _():
            self.run_in(k, which).start()

    def total_in(self, k, which):
        place = self.quarter(k, which)

        @pl.when(self.centre)
        def _():
            self.hand_on(5, 6, k, place, self.inward).start()

        @pl.when(self.inner)
        def _():
            self.hand_on(5, 5, k, place, self.inward).start()

    def stage(self, number, k):
        even, odd, centre, inner, outer, end = (
            self.even,
            self.odd,
            self.centre,
            self.inner,
            self.outer,
            self.end,
        )
        own, rest = self.chip, 1 - self.chip
        to_out, to_in = self.side, 1 - self.side
        mine, half = self.quarter(k, own), self.half(k)

        def when(*conditions):
            return pl.when(functools.reduce(jnp.logical_and, conditions))

        if number == 0:
            self.over_core(k).start()
        if number == 1:
            self.over_core(k).wait_recv()
            self.add(k, half, self.near, 2)

            @when(even)
            def _():
                self.over_chip(k, rest).start()

            @when(odd, end)
            def _():
                self.send_in(k, to_in)

        if number == 2:

            @when(even)
            def _():
                self.over_chip(k, rest).wait_recv()
                self.add(k, mine, self.across, 4)

            @when(even, end)
            def _():
                self.send_in(k, own)

            @when(odd, outer)
            def _():
                self.run_in(k, to_in).wait_recv()
                self.add(k, self.quarter(k, to_in), self.inflow, 4)
                self.send_in(k, to_in)

        if number == 3:

            @when(even, outer)
            def _():
                self.run_in(k, own).wait_recv()
                self.add(k, mine, self.inflow, 4)
                self.send_in(k, own)

            @when(odd, outer)
            def _():
                self.swap(k, to_out).wait_recv()
                self.add(k, self.quarter(k, to_out), self.middle, 4)
                self.run_out(k, to_out).start()

        if number == 4:

            @when(even, centre)
            def _():
                self.swap(k, own).wait_recv()
                self.add(k, mine, self.middle, 4, self.totals)
                self.hand_on(5, 5, k, mine, self.to_chip).start()

            @when(even, centre, outer)
            def _():
                self.hand_on(4, 4, k, mine, self.outward).start()

            @when(odd, end)
            def _():
                self.swap(k, to_out).wait_recv()
                self.add(k, self.quarter(k, to_out), self.middle, 4)
                self.over_chip(k, to_out).start()

        if number == 5:

            @when(even, inner)
            def _():
                self.hand_on(4, 4, k, mine, self.inward).wait_recv()
                self.hand_on(5, 5, k, mine, self.to_chip).start()

            @when(even, inner, outer)
            def _():
                self.hand_on(4, 4, k, mine, self.outward).start()

            @when(odd, end)
            def _():
                self.over_chip(k, to_out).wait_recv()
                self.add(k, self.quarter(k, to_out), self.across, 4, self.totals)
                self.total_in(k, to_out)

        if number == 6:

            @when(even)
            def _():
                self.hand_on(5, 5, k, self.quarter(k, rest), self.to_chip).wait_recv()
                self.hand_on(7, 7, k, half, self.to_core).start()

            @when(odd, outer)
            def _():
                self.hand_on(5, 5, k, self.quarter(k, to_out), self.inward).wait_recv()
                self.total_in(k, to_out)

        if number == 7:

            @when(odd, outer)
            def _():
                self.hand_on(6, 6, k, self.quarter(k, to_in), self.outward).wait_recv()
                self.hand_on(6, 6, k, self.quarter(k, to_in), self.outward).start()
                self.hand_on(7, 7, k, half, self.to_core).start()

        if number == 8:

            @when(odd, end)
            def _():
                self.hand_on(6, 6, k, self.quarter(k, to_in), self.inward).wait_recv()
                self.hand_on(7, 7, k, half, self.to_core).start()

        if number == 9:
            self.hand_on(7, 7, k, self.half(k, 1 - self.core), self.to_core).wait_recv()

    def settle(self, k):
        own, mine = self.quarter(k, self.chip), self.quarter(k, self.chip)
        self.over_core(k).wait_send()
        self.hand_on(7, 7, k, self.half(k), self.to_core).wait_send()

        def when(*conditions):
            return pl.when(functools.reduce(jnp.logical_and, conditions))

        @when(self.even)
        def _():
            self.over_chip(k, 1 - self.chip).wait_send()
            self.hand_on(5, 5, k, mine, self.to_chip).wait_send()

        @when(self.even, self.outer)
        def _():
            self.hand_on(4, 4, k, mine, self.outward).wait_send()

        @when(self.centre)
        def _():
            self.swap(k, 0).wait_send()

        @when(self.inner)
        def _():
            self.run_in(k, 0).wait_send()

        @when(self.odd)
        def _():
            self.hand_on(5, 5, k, own, self.inward).wait_send()

        @when(self.odd, self.end)
        def _():
            self.over_chip(k, 0).wait_send()

        @when(self.odd, self.outer)
        def _():
            self.run_out(k, 0).wait_send()
            self.hand_on(6, 6, k, own, self.outward).wait_send()


STAGES = 10
BACK, GATHER, LEAVE, FINISH, WEIGH = range(STAGES, STAGES + 5)
LAGS = (0, 1, 3, 5, 7, 9, 11, 12, 14, 15)


def order(layout, chunks):
    early = sum(name in ("down", "up") for name, _, _, _ in layout.subs)
    back = [3 + 1.5 * index for index in range(chunks)]
    ready = back[-1] + 0.5
    items = [(at, 0, BACK, index) for index, at in enumerate(back)]
    items.append((ready - 0.02, 0, GATHER, 0))
    items += [(ready + 5, index, LEAVE, index) for index in range(chunks)]
    items += [(ready + 8 + index, 0, FINISH, index) for index in range(chunks)]
    for k in range(len(layout.subs)):
        at = k if k < early else max(early, ready) + k - early
        items.append((at - 0.01, 0, WEIGH, k))
        items += [(at + lag, STAGES - stage, stage, k) for stage, lag in enumerate(LAGS)]
    return [(step, index) for _, _, step, index in sorted(items)]


def layer_kernel(
    length_ref,
    tokens_hbm,
    wqkv_hbm,
    wout_hbm,
    gain_one_ref,
    bias_one_ref,
    wup_hbm,
    wdown_hbm,
    gain_two_ref,
    bias_two_ref,
    cot_hbm,
    out_hbm,
    grad_hbm,
    sums_hbm,
    tokens,
    cot,
    wqkv,
    wout,
    wup,
    wdown,
    packed,
    probs,
    attended,
    mine,
    theirs,
    unit_one,
    inv_one,
    normed,
    normed_low,
    slope,
    activated,
    grad_up_in,
    grad_res,
    grad_low,
    grad_att,
    grad_key,
    grad_val,
    grad_packed,
    small,
    parts,
    totals,
    near,
    across,
    inflow,
    middle,
    in_sem,
    out_sem,
    send_sem,
    recv_sem,
    sums_sem,
    sums_send,
    sums_recv,
    *,
    layout,
):
    rows, width = tokens.shape
    hidden = wup.shape[1]
    cols = wout.shape[0]
    pairs = cols // 128
    chunks = rows // CHUNK
    scaling = HEAD_DIM**-0.5
    other = {"tp": 1 - lax.axis_index("tp")}

    total = Sum(layout, parts, totals, near, across, inflow, middle, sums_send, sums_recv)
    barrier = pltpu.get_barrier_semaphore()
    pl.semaphore_signal(barrier, 1, device_id=other, device_id_type=MESH)
    total.greet(barrier)

    loads = [
        pltpu.make_async_copy(source, target, in_sem.at[place])
        for place, (source, target) in enumerate(
            (
                (tokens_hbm, tokens),
                (wqkv_hbm, wqkv),
                (wout_hbm, wout),
                (wup_hbm, wup),
                (wdown_hbm, wdown),
                (cot_hbm, cot),
            )
        )
    ]
    for load in loads:
        load.start()

    def at(index):
        return pl.ds(pl.multiple_of(index * CHUNK, CHUNK), CHUNK)

    def exchange(which, index):
        return pltpu.make_async_remote_copy(
            src_ref=mine.at[which, at(index)],
            dst_ref=theirs.at[which, at(index)],
            send_sem=send_sem.at[which, index],
            recv_sem=recv_sem.at[which, index],
            device_id=other,
            device_id_type=MESH,
        )

    def received(which, index):
        place = at(index)
        return mine[which, place, :].astype(F32) + theirs[which, place, :].astype(F32)

    small[...] = jnp.zeros_like(small)
    grad_key[...] = jnp.zeros_like(grad_key)
    grad_val[...] = jnp.zeros_like(grad_val)

    lane = lax.broadcasted_iota(jnp.int32, (1, 128), 1)
    first = jnp.where(lane < HEAD_DIM, 1.0, 0.0).astype(BF16)
    second = jnp.where(lane < HEAD_DIM, 0.0, 1.0).astype(BF16)
    live = lax.broadcasted_iota(jnp.int32, (1, rows), 1) < length_ref[0]

    def stacked(block):
        return jnp.concatenate([block * first, block * second], axis=0)

    def merged(both):
        return jnp.where(lane < HEAD_DIM, both[:CHUNK], both[CHUNK:])

    gain_one_row = gain_one_ref[...].reshape(1, width)
    bias_one_row = bias_one_ref[...].reshape(1, width)
    gain_two_row = gain_two_ref[...].reshape(1, width)
    bias_two_row = bias_two_ref[...].reshape(1, width)

    loads[0].wait()
    loads[1].wait()

    def project(index, carry):
        place = at(index)
        for part in range(3):
            value = dot(tokens[place, :], wqkv[part], 1, 0).astype(BF16)
            packed[part, place, :] = value * BF16(scaling) if part == 0 else value
        return carry

    lax.fori_loop(0, chunks, project, 0)
    loads[2].wait()
    total.meet(barrier, 1)

    def attend(index, carry):
        place = at(index)
        for pair in range(pairs):
            span = slice(pair * 128, pair * 128 + 128)
            scores = dot(stacked(packed[0, place, span]), packed[1, :, span], 1, 1)
            scores = jnp.where(live, scores, -1000000000.0)
            expo = jnp.exp(scores - jnp.max(scores, axis=-1, keepdims=True))
            weight = jnp.sum(expo, axis=-1, keepdims=True)
            low = (expo * (1.0 / weight)).astype(BF16)
            probs[pair * chunks + index] = low
            attended[place, span] = merged(dot(low, packed[2, :, span], 1, 0)).astype(BF16)
        mine[0, place, :] = dot(attended[place, :], wout[...], 1, 0).astype(BF16)
        exchange(0, index).start()
        return carry

    lax.fori_loop(0, chunks, attend, 0)
    loads[3].wait()
    loads[4].wait()
    loads[5].wait()

    def feed(index, carry):
        place = at(index)
        exchange(0, index).wait()
        unit, inverse = norm_forward(tokens[place, :].astype(F32) + received(0, index))
        unit_one[place, :] = unit
        inv_one[place, :] = inverse
        value = unit * gain_one_row + bias_one_row
        normed[place, :] = value
        normed_low[place, :] = value.astype(BF16)
        for start in range(0, hidden, SUB):
            span = slice(start, start + SUB)
            upward = dot(normed_low[place, :], wup[:, span], 1, 0)
            share = 0.5 + 0.5 * lax.erf(upward * 0.7071067811865476)
            activated[place, span] = (upward * share).astype(BF16)
            slope[place, span] = share + upward * jnp.exp(upward * upward * -0.5) * 0.3989422804014327
        mine[1, place, :] = dot(activated[place, :], wdown[...], 1, 0).astype(BF16)
        exchange(1, index).start()
        return carry

    lax.fori_loop(0, chunks, feed, 0)

    def turn(index, carry):
        place = at(index)
        exchange(1, index).wait()
        unit, inverse = norm_forward(normed[place, :] + received(1, index))
        mine[4, place, :] = (unit * gain_two_row + bias_two_row).astype(BF16)
        pltpu.make_async_copy(mine.at[4, place], out_hbm.at[place], out_sem.at[0, index]).start()
        flow = cot[place, :].astype(F32)
        small[2:3, :] += jnp.sum(flow * unit, axis=0, keepdims=True)
        small[3:4, :] += jnp.sum(flow, axis=0, keepdims=True)
        grad = norm_backward(flow * gain_two_row, unit, inverse)
        grad_res[place, :] = grad
        grad_low[0, place, :] = grad.astype(BF16)
        for start in range(0, hidden, SUB):
            span = slice(start, start + SUB)
            grad_act = dot(grad_low[0, place, :], wdown[span, :], 1, 1)
            grad_up_in[place, span] = (grad_act * slope[place, span]).astype(BF16)
        mine[2, place, :] = dot(grad_up_in[place, :], wup[...], 1, 1).astype(BF16)
        exchange(2, index).start()
        return carry

    lax.fori_loop(0, chunks, turn, 0)

    def attend_back(index):
        place = at(index)
        exchange(2, index).wait()
        unit = unit_one[place, :]
        flow = grad_res[place, :] + received(2, index)
        small[0:1, :] += jnp.sum(flow * unit, axis=0, keepdims=True)
        small[1:2, :] += jnp.sum(flow, axis=0, keepdims=True)
        grad = norm_backward(flow * gain_one_row, unit, inv_one[place, :])
        grad_res[place, :] = grad
        grad_low[1, place, :] = grad.astype(BF16)
        grad_att[place, :] = dot(grad_low[1, place, :], wout[...], 1, 1).astype(BF16)
        for pair in range(pairs):
            span = slice(pair * 128, pair * 128 + 128)
            low = probs[pair * chunks + index]
            pull = stacked(grad_att[place, span])
            seen = attended[place, span].astype(F32)
            centre = jnp.sum(
                pull.astype(F32) * jnp.concatenate([seen, seen], axis=0), axis=-1, keepdims=True
            )
            grad_probs = dot(pull, packed[2, :, span], 1, 1)
            grad_scores = (low.astype(F32) * (grad_probs - centre)).astype(BF16)
            grad_val[:, span] += dot(low, pull, 0, 0)
            grad_key[:, span] += dot(grad_scores, stacked(packed[0, place, span]), 0, 0)
            grad_query = merged(dot(grad_scores, packed[1, :, span], 1, 0)) * scaling
            grad_packed[0, place, span] = grad_query.astype(BF16)

    def gather():
        grad_packed[1] = grad_key[...].astype(BF16)
        grad_packed[2] = grad_val[...].astype(BF16)

    def leave(index):
        place = at(index)
        value = dot(grad_packed[0, place, :], wqkv[0], 1, 1)
        value += dot(grad_packed[1, place, :], wqkv[1], 1, 1)
        value += dot(grad_packed[2, place, :], wqkv[2], 1, 1)
        mine[3, place, :] = value.astype(BF16)
        exchange(3, index).start()

    def weigh(k):
        name, which, start, extent = layout.subs[k]
        if name == "down":
            rows_at = which * SUB
            value = dot(activated[:, rows_at : rows_at + SUB], grad_low[0], 0, 0)
            parts[start : start + SUB, :] = value.astype(BF16)
        if name == "up":
            rows_at, cols_at = which % 2 * SUB, which // 2 * width
            left = normed_low[:, rows_at : rows_at + SUB]
            value = dot(left, grad_up_in[:, cols_at : cols_at + width], 0, 0)
            parts[start : start + SUB, :] = value.astype(BF16)
        if name == "out":
            parts[start : start + SUB, :] = dot(attended[...], grad_low[1], 0, 0).astype(BF16)
            parts[start + SUB : start + extent, :] = small[...].astype(BF16)
        if name == "qkv":
            span = slice(which * 128, which * 128 + 128)
            for part in range(3):
                value = dot(tokens[...], grad_packed[part, :, span], 0, 0).astype(BF16)
                for side in range(2):
                    left = side * SUB + part * 128
                    rows_at = side * SUB
                    parts[start : start + SUB, left : left + 128] = value[rows_at : rows_at + SUB]

    def finish(index):
        place = at(index)
        exchange(3, index).wait()
        mine[5, place, :] = (grad_res[place, :] + received(3, index)).astype(BF16)
        pltpu.make_async_copy(mine.at[5, place], grad_hbm.at[place], out_sem.at[1, index]).start()

    def store(k):
        _, _, start, extent = layout.subs[k]
        place = pl.ds(start, extent)
        return pltpu.make_async_copy(totals.at[place], sums_hbm.at[place], sums_sem.at[k])

    for step, index in order(layout, chunks):
        if step == BACK:
            attend_back(index)
        elif step == GATHER:
            gather()
        elif step == LEAVE:
            leave(index)
        elif step == FINISH:
            finish(index)
        elif step == WEIGH:
            weigh(index)
        else:
            total.stage(step, index)
            if step == STAGES - 1:
                store(index).start()

    for index in range(chunks):
        place = at(index)
        pltpu.make_async_copy(mine.at[4, place], out_hbm.at[place], out_sem.at[0, index]).wait()
        pltpu.make_async_copy(mine.at[5, place], grad_hbm.at[place], out_sem.at[1, index]).wait()
    for k in range(len(layout.subs)):
        total.settle(k)
        store(k).wait()


def widen_kernel(
    sums_hbm,
    out_in,
    grad_in,
    out_hbm,
    grad_hbm,
    qkv_hbm,
    wout_hbm,
    gain_one_hbm,
    bias_one_hbm,
    up_hbm,
    down_hbm,
    gain_two_hbm,
    bias_two_hbm,
    sums,
    wide,
    vectors,
    rows_in,
    in_sem,
    out_sem,
    row_sem,
    *,
    layout,
):
    slots = wide.shape[0]
    width = sums.shape[1]

    def load(k):
        _, _, start, rows = layout.subs[k]
        return pltpu.make_async_copy(
            sums_hbm.at[pl.ds(start, rows)], sums.at[pl.ds(start, rows)], in_sem.at[k]
        )

    def stores(k):
        name, which, _, _ = layout.subs[k]
        slot = k % slots
        block = wide.at[slot, pl.ds(0, SUB)]
        if name == "down":
            pieces = [(block, down_hbm.at[pl.ds(which * SUB, SUB)])]
        elif name == "up":
            pieces = [
                (block, up_hbm.at[pl.ds(which % 2 * SUB, SUB), pl.ds(which // 2 * width, width)])
            ]
        elif name == "out":
            pieces = [(block, wout_hbm)]
            for row, target in enumerate((gain_one_hbm, bias_one_hbm, gain_two_hbm, bias_two_hbm)):
                pieces.append((vectors.at[row], target))
        else:
            pieces = [
                (
                    wide.at[slot, pl.ds(0, SUB), pl.ds(half * SUB + part * 128, 128)],
                    qkv_hbm.at[part, pl.ds(half * SUB, SUB), pl.ds(which * 128, 128)],
                )
                for half in range(2)
                for part in range(3)
            ]
        return [
            pltpu.make_async_copy(source, target, out_sem.at[slot, place])
            for place, (source, target) in enumerate(pieces)
        ]

    through = ((out_in, out_hbm), (grad_in, grad_hbm))
    for place, (source, _) in enumerate(through):
        pltpu.make_async_copy(source, rows_in.at[place], row_sem.at[place]).start()
    for k in range(len(layout.subs)):
        load(k).start()
    for place, (source, target) in enumerate(through):
        pltpu.make_async_copy(source, rows_in.at[place], row_sem.at[place]).wait()
        pltpu.make_async_copy(rows_in.at[place], target, row_sem.at[2 + place]).start()
    for k, (name, _, start, _) in enumerate(layout.subs):
        load(k).wait()
        if k >= slots:
            for store in stores(k - slots):
                store.wait()
        wide[k % slots, 0:SUB, :] = sums[start : start + SUB, :].astype(F32)
        if name == "out":
            low = sums[start + SUB : start + SUB + 16, :].astype(F32)
            for row in range(4):
                vectors[row] = low[row]
        for store in stores(k):
            store.start()
    for k in range(len(layout.subs) - slots, len(layout.subs)):
        for store in stores(k):
            store.wait()
    for place, (_, target) in enumerate(through):
        pltpu.make_async_copy(rows_in.at[place], target, row_sem.at[2 + place]).wait()


def on_device(
    tokens,
    lengths,
    weight_qkv,
    weight_out,
    gain_one,
    bias_one,
    weight_up,
    weight_down,
    gain_two,
    bias_two,
    cotangent,
):
    seq_count, rows, width = tokens.shape
    cols, hidden = weight_out.shape[0], weight_up.shape[1]
    assert seq_count == 1 and rows % CHUNK == 0 and lax.axis_size("tp") == 2
    layout = Layout(width, cols, hidden)
    count = len(layout.subs)
    chunks = rows // CHUNK
    pairs = cols // 128
    whole = pl.BlockSpec(memory_space=pltpu.VMEM)
    out_rows, grad_rows, sums = pl.pallas_call(
        functools.partial(layer_kernel, layout=layout),
        name="layer",
        out_shape=(
            jax.ShapeDtypeStruct((rows, width), BF16),
            jax.ShapeDtypeStruct((rows, width), BF16),
            jax.ShapeDtypeStruct((layout.rows, width), BF16),
        ),
        in_specs=[
            pl.BlockSpec(memory_space=pltpu.SMEM),
            ANY,
            ANY,
            ANY,
            whole,
            whole,
            ANY,
            ANY,
            whole,
            whole,
            ANY,
        ],
        out_specs=(ANY, ANY, ANY),
        scratch_shapes=[
            pltpu.VMEM((rows, width), BF16),
            pltpu.VMEM((rows, width), BF16),
            pltpu.VMEM((3, width, cols), BF16),
            pltpu.VMEM((cols, width), BF16),
            pltpu.VMEM((width, hidden), BF16),
            pltpu.VMEM((hidden, width), BF16),
            pltpu.VMEM((3, rows, cols), BF16),
            pltpu.VMEM((pairs * chunks, 2 * CHUNK, rows), BF16),
            pltpu.VMEM((rows, cols), BF16),
            pltpu.VMEM((6, rows, width), BF16),
            pltpu.VMEM((4, rows, width), BF16),
            pltpu.VMEM((rows, width), F32),
            pltpu.VMEM((rows, 1), F32),
            pltpu.VMEM((rows, width), F32),
            pltpu.VMEM((rows, width), BF16),
            pltpu.VMEM((rows, hidden), F32),
            pltpu.VMEM((rows, hidden), BF16),
            pltpu.VMEM((rows, hidden), BF16),
            pltpu.VMEM((rows, width), F32),
            pltpu.VMEM((2, rows, width), BF16),
            pltpu.VMEM((rows, cols), BF16),
            pltpu.VMEM((rows, cols), F32),
            pltpu.VMEM((rows, cols), F32),
            pltpu.VMEM((3, rows, cols), BF16),
            pltpu.VMEM((SMALL, width), F32),
            pltpu.VMEM((layout.rows, width), BF16),
            pltpu.VMEM((layout.rows, width), BF16),
            pltpu.VMEM((layout.rows // 2, width), BF16),
            pltpu.VMEM((layout.rows // 4, width), BF16),
            pltpu.VMEM((layout.rows // 4, width), BF16),
            pltpu.VMEM((layout.rows // 4, width), BF16),
            pltpu.SemaphoreType.DMA((6,)),
            pltpu.SemaphoreType.DMA((2, chunks)),
            pltpu.SemaphoreType.DMA((4, chunks)),
            pltpu.SemaphoreType.DMA((4, chunks)),
            pltpu.SemaphoreType.DMA((count,)),
            pltpu.SemaphoreType.DMA((8, count)),
            pltpu.SemaphoreType.DMA((8, count)),
        ],
        compiler_params=pltpu.CompilerParams(
            collective_id=1, has_side_effects=True, vmem_limit_bytes=VMEM_LIMIT
        ),
    )(
        lengths,
        tokens.reshape(rows, width),
        jnp.transpose(weight_qkv, (1, 0, 2)),
        weight_out,
        gain_one,
        bias_one,
        weight_up,
        weight_down,
        gain_two,
        bias_two,
        cotangent.reshape(rows, width),
    )
    vector = jax.ShapeDtypeStruct((width,), F32)
    results = pl.pallas_call(
        functools.partial(widen_kernel, layout=layout),
        name="widen",
        out_shape=(
            jax.ShapeDtypeStruct((rows, width), BF16),
            jax.ShapeDtypeStruct((rows, width), BF16),
            jax.ShapeDtypeStruct((3, width, cols), F32),
            jax.ShapeDtypeStruct((cols, width), F32),
            vector,
            vector,
            jax.ShapeDtypeStruct((width, hidden), F32),
            jax.ShapeDtypeStruct((hidden, width), F32),
            vector,
            vector,
        ),
        in_specs=[ANY] * 3,
        out_specs=(ANY,) * 10,
        scratch_shapes=[
            pltpu.VMEM((layout.rows, width), BF16),
            pltpu.VMEM((4, SUB, width), F32),
            pltpu.VMEM((4, width), F32),
            pltpu.VMEM((2, rows, width), BF16),
            pltpu.SemaphoreType.DMA((count,)),
            pltpu.SemaphoreType.DMA((4, 6)),
            pltpu.SemaphoreType.DMA((4,)),
        ],
        compiler_params=pltpu.CompilerParams(vmem_limit_bytes=VMEM_LIMIT),
    )(sums, out_rows, grad_rows)
    return (
        results[0].reshape(seq_count, rows, width),
        results[1].reshape(seq_count, rows, width),
        jnp.transpose(results[2], (1, 0, 2)),
        results[3],
        results[4],
        results[5],
        results[6],
        results[7],
        results[8],
        results[9],
    )


def solution(mesh):
    batch = P(("dp", "dq"), None, None)
    return jax.shard_map(
        on_device,
        mesh=mesh,
        in_specs=(
            batch,
            P(("dp", "dq")),
            P(None, None, "tp"),
            P("tp", None),
            P(),
            P(),
            P(None, "tp"),
            P("tp", None),
            P(),
            P(),
            batch,
        ),
        out_specs=(
            batch,
            batch,
            P(None, None, "tp"),
            P("tp", None),
            P(),
            P(),
            P(None, "tp"),
            P("tp", None),
            P(),
            P(),
        ),
        check_vma=False,
    )
```
